1024 devices in a mesh: grid: 64 (over x, z_hi, y), band: 16 (over z_lo, core).
Axes of the slice: x: 4, y: 4, z: 32 (z_hi: 4, z_lo: 8; z = z_hi * 8 + z_lo), core: 2. Of those that a mesh axis runs over, the one named last changes fastest.
Arguments:
- orbitals: bfloat16 [128, 64, 64, 128], P('band', 'grid'), may hold values from -6 to 6
- occupation: int32 [128], P('band'), may hold values from 1 to 2
- spin_of_band: int32 [128], P('band'), may hold values from 0 to 1
- ionic_charge: float32 [64, 64, 128], P('grid'), may hold values from 0.3 to 3
Outputs:
- potential: float32 [2, 64, 64, 128], P(None, 'grid')
- applied: bfloat16 [128, 64, 64, 128], P('band', 'grid')
The draws below stay inside these ranges and needn't reach their ends.
All inputs are finite; a program needn't handle non-finite values.
Results may differ from the reference program's by a relative error of at most 0.001.
Values sent between devices are 32-bit elements; how exact they have to be, the bound alone decides.
A program may use at most 32 MiB of HBM per device.

```python
import math
import jax
import jax.numpy as jnp
from jax import lax

NX = 128
NY = 64
NZ = 64
BANDS = 128


def with_ends(entries, rng, smallest, largest):
    shape = entries.shape
    spot = [jax.random.randint(jax.random.fold_in(rng, axis), (), 0, shape[axis]) for axis in range(len(shape))]
    entries = entries.at[tuple(spot)].set(smallest)
    longest = shape.index(max(shape))
    spot[longest] = (spot[longest] + 1) % shape[longest]
    return entries.at[tuple(spot)].set(largest)


def block_levels(stream_key, dims, shards, low, high):
    def one(position, parts):
        draws = jax.random.uniform(jax.random.fold_in(jax.random.fold_in(stream_key, 6), position), (parts,), jnp.float32, low / len(shards), high / len(shards))
        return jnp.repeat(jnp.exp(draws), dims[position] // parts).reshape((-1,) + (1,) * (len(dims) - position - 1))

    level = one(*shards[0])
    for cut in shards[1:]:
        level = level * one(*cut)
    return level


def noise(rng, extent, width, most, pieces=(), kind=jnp.bfloat16):
    entries = jax.random.normal(rng, extent, jnp.float32) * width
    if len(pieces) > 0:
        entries = block_levels(rng, extent, pieces, -0.22, 0.18) * entries
    return jnp.clip(entries, min=-most, max=most).astype(kind)


def setup_inputs(seed: int = 0) -> dict:
    key_of = jax.random.split(jax.random.key(seed), 5)
    return {
        "orbitals": noise(key_of[0], (BANDS, NZ, NY, NX), 1.0, 6.0, ((0, 16), (1, 64))),
        "occupation": with_ends(jax.random.randint(key_of[1], (BANDS,), 1, 3), jax.random.fold_in(key_of[1], 1), 1, 2).astype(jnp.int32),
        "spin_of_band": with_ends(jax.random.randint(key_of[2], (BANDS,), 0, 2), jax.random.fold_in(key_of[2], 1), 0, 1).astype(jnp.int32),
        "ionic_charge": jnp.clip(jnp.exp(math.log(3.0) - 2.3025851 * jax.random.uniform(key_of[3], (NZ, NY, NX), jnp.float32) ** block_levels(key_of[3], (NZ, NY, NX), ((0, 64),), -0.2, 0.2)), 0.3, 3.0),
    }


spacing = 0.25


def signed_sq(count):
    index = jnp.arange(count, dtype=jnp.int32)
    signed = jnp.where(index < count // 2, index, index - count).astype(jnp.float32)
    wave = 2.0 * math.pi * signed / (count * spacing)
    return wave * wave


def reference(orbitals, occupation, spin_of_band, ionic_charge):
    total = orbitals.shape[0]
    channels = jnp.arange(2, dtype=jnp.int32)
    weights = jnp.where(spin_of_band[None, :] == channels[:, None], occupation[None, :].astype(jnp.float32), jnp.float32(0.0)) / total

    def accumulate(acc, pair):
        column, orbital = pair
        square = orbital.astype(jnp.float32) * orbital.astype(jnp.float32)
        return acc + column[:, None, None, None] * square[None], None

    start = jnp.zeros((2,) + orbitals.shape[1:], jnp.float32)
    density, unused = lax.scan(accumulate, start, (weights.T, orbitals))
    exchange = -jnp.cbrt(6.0 / math.pi * density)
    net = density[0] + density[1] - ionic_charge
    nz, ny, nx = net.shape
    g_sq = signed_sq(nz)[:, None, None] + signed_sq(ny)[None, :, None] + signed_sq(nx)[None, None, :]
    kernel = jnp.where(g_sq > 0, 4.0 * math.pi / jnp.where(g_sq > 0, g_sq, 1.0), 0.0)
    hartree = jnp.real(jnp.fft.ifftn(jnp.fft.fftn(net) * kernel)).astype(jnp.float32)
    potential = hartree[None] + exchange

    def apply_one(pair):
        channel, orbital = pair
        return (potential[channel] * orbital.astype(jnp.float32)).astype(jnp.bfloat16)

    applied = lax.map(apply_one, (spin_of_band, orbitals))
    return potential, applied
```

```python
import functools
import math

import jax
import jax.numpy as jnp
import numpy as np
from jax import lax
from jax.experimental import pallas as pl
from jax.experimental.pallas import tpu as pltpu
from jax.sharding import PartitionSpec as P

X, H, Y, L = 4, 4, 4, 8
SPACING = 0.25
MESH = pl.DeviceIdType.MESH
HIGHEST = lax.Precision.HIGHEST


def cas(count):
    index = np.arange(count)
    angle = 2.0 * np.pi * ((index[:, None] * index[None, :]) % count) / count
    return (np.cos(angle) + np.sin(angle)).astype(np.float32)


def wave_sq(count):
    index = np.arange(count)
    signed = np.where(index < count // 2, index, index - count)
    return (2.0 * np.pi * signed / (count * SPACING)) ** 2


def green(depth, rows, cols):
    g_sq = wave_sq(depth)[:, None, None] + wave_sq(rows)[None, :, None] + wave_sq(cols)[None, None, :]
    kernel = np.where(g_sq > 0, 4.0 * np.pi / np.where(g_sq > 0, g_sq, 1.0), 0.0)
    index = np.arange(depth)
    cos_z = np.cos(2.0 * np.pi * ((index[:, None] * index[None, :]) % depth) / depth)
    table = np.tensordot(cos_z, kernel, 1) / (depth * rows * cols)
    share = rows // L
    return np.ascontiguousarray(
        table.reshape(depth, L, share, cols).transpose(1, 0, 2, 3).astype(np.float32)
    )


def dot(a, b):
    return jnp.dot(a, b, precision=HIGHEST, preferred_element_type=jnp.float32)


def wrap(value, count):
    return lax.rem(value + count, count)


def field_kernel(
    total,
    occ, spin, orb_hbm, ion_hbm, hx_hbm, hy_hbm, g_hbm,
    out,
    orb, ion, hx, hy, gz,
    d_own, t_own, t_in, d_in,
    spec, ra, pb, rb, cs, rc, vb, rd, hart, ex_in,
    ds, rr, es, ex, h_in,
    load_sem, send, recv,
):
    rows = hy.shape[0]
    share = rows // L
    ring = H * L
    half = L // 2
    depth = X * H * Y
    g, b = lax.axis_index("grid"), lax.axis_index("band")
    x, h, y = lax.div(g, H * Y), lax.rem(lax.div(g, Y), H), lax.rem(g, Y)
    l, c = lax.div(b, 2), lax.rem(b, 2)
    p = h * L + l
    side = 2 * lax.div(l, half) - 1

    def at(dx, dy, place, core):
        row = (wrap(x + dx, X) * H + lax.div(place, L)) * Y + wrap(y + dy, Y)
        return (row, lax.rem(place, L) * 2 + core)

    partner = (g, b + 1 - 2 * c)
    window = [o for o in range(-half, half + 1) if o != 0]
    inward = [o for o in range(-half, half) if o != 0]
    others = [(dx, dy) for dx in range(X) for dy in range(Y) if dx + dy > 0]

    loads = [
        pltpu.make_async_copy(src, dst, load_sem.at[i])
        for i, (src, dst) in enumerate(
            [(orb_hbm, orb), (ion_hbm, ion), (hx_hbm, hx), (hy_hbm, hy), (g_hbm.at[l], gz)]
        )
    ]
    for load in loads:
        load.start()

    barrier = pltpu.get_barrier_semaphore()

    def greet(device):
        pl.semaphore_signal(barrier, inc=1, device_id=device, device_id_type=MESH)

    greet(partner)

    @pl.when(c == 1)
    def _():
        for o in window:
            greet(at(0, 0, wrap(p + o, ring), 1))
        for j in range(1, H):
            greet(at(0, 0, wrap(p + j * L, ring), 1))
        for dx, dy in others:
            greet(at(dx, dy, p, 1))

    @pl.when(c == 0)
    def _():
        for j in range(1, L):
            greet(at(0, 0, h * L + lax.rem(l + j, L), 0))

    loads[0].wait()
    w = [occ[i].astype(jnp.float32) / total for i in range(orb.shape[0])]
    up = [spin[i].astype(jnp.float32) for i in range(orb.shape[0])]
    d0 = jnp.zeros(t_own.shape, jnp.float32)
    d1 = jnp.zeros(t_own.shape, jnp.float32)
    for i in range(orb.shape[0]):
        value = orb[i].astype(jnp.float32)
        square = value * value
        d0 = d0 + (w[i] * (1.0 - up[i])) * square
        d1 = d1 + (w[i] * up[i]) * square
    d_own[0] = d0
    d_own[1] = d1
    t_own[...] = d0 + d1

    for load in loads[1:]:
        load.wait()

    def remote(src, dst, phase, device):
        return pltpu.make_async_remote_copy(
            src_ref=src, dst_ref=dst, send_sem=send.at[phase], recv_sem=recv.at[phase],
            device_id=device, device_id_type=MESH,
        )

    def arrived(like, phase):
        remote(like, like, phase, partner).wait_recv()

    def sent(like, phase):
        remote(like, like, phase, partner).wait_send()

    @pl.when(c == 1)
    def _():
        pl.semaphore_wait(barrier, 1 + len(window) + H - 1 + len(others))
        remote(d_own, d_in, 0, partner).start()
        arrived(t_in, 1)
        charge = t_own[...] + t_in[...] - ion[...] * (1.0 / L)
        spec[...] = dot(dot(hy[...], charge), hx[...])
        for o in sorted(inward, key=abs, reverse=True):
            place = wrap(p - o, ring)
            rows_of = pl.ds(pl.multiple_of(lax.rem(place, L) * share, share), share)
            remote(spec.at[rows_of], ra.at[inward.index(o)], 2, at(0, 0, place, 1)).start()
        own = spec[pl.ds(pl.multiple_of(l * share, share), share), :]
        arrived(ra, 2)
        other = jnp.zeros_like(own)
        for slot, o in enumerate(inward):
            block = ra[slot]
            mine = lax.div(wrap(p + o, ring), L) == h
            own = own + jnp.where(mine, block, 0.0)
            other = other + jnp.where(mine, 0.0, block)
        pb[0] = own
        pb[1] = other
        for j in sorted(range(1, H), key=lambda j: -min(j, H - j)):
            remote(pb, rb.at[j - 1], 3, at(0, 0, wrap(p + j * L, ring), 1)).start()
        arrived(rb, 3)
        first = [pb[0]] + [rb[j - 1, 0] for j in range(1, H)]
        second = [pb[1]] + [rb[j - 1, 1] for j in range(1, H)]
        left = side < 0
        planes = [
            first[j] + jnp.where(left, second[(j - 1) % H], second[(j + 1) % H]) for j in range(H)
        ]

        def response(dx, dy, t):
            tx, ty, th = wrap(x + dx, X), wrap(y + dy, Y), wrap(h + t * side, H)
            target = (tx * H + th) * Y + ty
            value = None
            for j in range(H):
                source = (x * H + wrap(h - j, H)) * Y + y
                term = gz[wrap(target - source, depth)] * planes[j]
                value = term if value is None else value + term
            return value

        hops = lambda d: min(d[0], X - d[0]) + min(d[1], Y - d[1])
        for dx, dy in sorted(others, key=hops, reverse=True):
            slot = others.index((dx, dy))
            for t in range(2):
                cs[slot, t] = response(dx, dy, t)
            remote(cs.at[slot], rc.at[slot], 4, at(dx, dy, p, 1)).start()
        now = [response(0, 0, t) for t in range(2)]
        arrived(rc, 4)
        for slot in range(len(others)):
            now = [now[t] + rc[slot, t] for t in range(2)]
        vb[0] = now[0]
        vb[1] = now[1]
        mine_rows = pl.ds(pl.multiple_of(l * share, share), share)
        rd[mine_rows, :] = now[0]
        for o in sorted(inward, key=abs, reverse=True):
            place = wrap(p + o, ring)
            plane = lax.div(place, L)
            differs = (plane != h).astype(jnp.int32)
            remote(vb.at[differs], rd.at[mine_rows], 5, at(0, 0, place, 1)).start()
        arrived(rd.at[pl.ds(0, rows - share)], 5)
        hart[...] = dot(dot(hy[...], rd[...]), hx[...])
        remote(hart, h_in, 6, partner).start()
        arrived(ex_in, 7)
        out[0] = hart[...] + ex_in[0]
        out[1] = hart[...] + ex_in[1]
        sent(d_own, 0)
        sent(ra, 2)
        sent(rb, 3)
        sent(rc, 4)
        sent(rd.at[pl.ds(0, rows - share)], 5)
        sent(hart, 6)

    @pl.when(c == 0)
    def _():
        pl.semaphore_wait(barrier, L)
        remote(t_own, t_in, 1, partner).start()
        arrived(d_in, 0)
        ds[...] = d_own[...] + d_in[...]
        for j in range(1, L):
            to = lax.rem(l + j, L)
            rows_of = pl.ds(pl.multiple_of(to * share, share), share)
            remote(ds.at[:, rows_of, :], rr.at[j - 1], 2, at(0, 0, h * L + to, 0)).start()
        mine_rows = pl.ds(pl.multiple_of(l * share, share), share)
        density = ds[:, mine_rows, :]
        arrived(rr, 2)
        for j in range(L - 1):
            density = density + rr[j]
        scaled = (6.0 / math.pi) * density
        positive = scaled > 0.0
        root = jnp.exp(jnp.log(jnp.where(positive, scaled, 1.0)) * (1.0 / 3.0))
        es[...] = jnp.where(positive, -root, 0.0)
        ex[:, mine_rows, :] = es[...]
        for j in range(1, L):
            to = lax.rem(l + j, L)
            remote(es, ex.at[:, mine_rows, :], 3, at(0, 0, h * L + to, 0)).start()
        arrived(rr, 3)
        remote(ex, ex_in, 7, partner).start()
        arrived(h_in, 6)
        out[0] = h_in[...] + ex[0]
        out[1] = h_in[...] + ex[1]
        sent(t_own, 1)
        sent(rr, 2)
        sent(rr, 3)
        sent(ex, 7)


def apply_kernel(spin, pot, orb, potential, applied):
    potential[...] = pot[...]
    for i in range(orb.shape[0]):
        chosen = jnp.where(spin[i] == 1, pot[1], pot[0])
        applied[i] = (chosen * orb[i].astype(jnp.float32)).astype(jnp.bfloat16)


def local(orbitals, occupation, spin_of_band, ionic_charge):
    bands, planes, rows, cols = orbitals.shape
    depth = X * H * Y
    share = rows // L
    total = bands * lax.axis_size("band")
    orb = orbitals.reshape(bands, rows, cols)
    f32 = jnp.float32
    plane, pair = (rows, cols), (2, rows, cols)
    vmem = lambda *shape: pltpu.VMEM(shape, f32)
    others = X * Y - 1
    hbm = pl.BlockSpec(memory_space=pl.ANY)
    smem = pl.BlockSpec(memory_space=pltpu.SMEM)
    invmem = pl.BlockSpec(memory_space=pltpu.VMEM)
    pot = pl.pallas_call(
        functools.partial(field_kernel, float(total)),
        out_shape=jax.ShapeDtypeStruct(pair, f32),
        in_specs=[smem, smem, hbm, hbm, hbm, hbm, hbm],
        out_specs=invmem,
        scratch_shapes=[
            pltpu.VMEM((bands, rows, cols), jnp.bfloat16),
            vmem(*plane), vmem(cols, cols), vmem(rows, rows), vmem(depth, share, cols),
            vmem(*pair), vmem(*plane), vmem(*plane), vmem(*pair),
            vmem(*plane), vmem(L - 1, share, cols), vmem(2, share, cols),
            vmem(H - 1, 2, share, cols), vmem(others, 2, share, cols), vmem(others, 2, share, cols),
            vmem(2, share, cols), vmem(*plane), vmem(*plane), vmem(*pair),
            vmem(*pair), vmem(L - 1, 2, share, cols), vmem(2, share, cols), vmem(*pair), vmem(*plane),
            pltpu.SemaphoreType.DMA((5,)),
            pltpu.SemaphoreType.DMA((8,)),
            pltpu.SemaphoreType.DMA((8,)),
        ],
        compiler_params=pltpu.CompilerParams(collective_id=0, has_side_effects=True),
        name="field",
    )(
        occupation, spin_of_band, orb, ionic_charge.reshape(rows, cols),
        jnp.asarray(cas(cols)), jnp.asarray(cas(rows)), jnp.asarray(green(depth, rows, cols)),
    )
    potential, applied = pl.pallas_call(
        apply_kernel,
        out_shape=(
            jax.ShapeDtypeStruct(pair, f32),
            jax.ShapeDtypeStruct((bands, rows, cols), jnp.bfloat16),
        ),
        in_specs=[smem, invmem, invmem],
        out_specs=(invmem, invmem),
        name="apply",
    )(spin_of_band, pot, orb)
    return (
        potential.reshape(2, planes, rows, cols),
        applied.reshape(bands, planes, rows, cols),
    )


def solution(mesh):
    return jax.shard_map(
        local,
        mesh=mesh,
        in_specs=(P("band", "grid", None, None), P("band"), P("band"), P("grid", None, None)),
        out_specs=(P(None, "grid", None, None), P("band", "grid", None, None)),
        check_vma=False,
    )
```
